32 devices in a mesh: clip: 16 (over z, y, x), mp: 2 (over core).
Axes of the slice: x: 2, y: 2, z: 4, core: 2. Of those that a mesh axis runs over, the one named last changes fastest.
Arguments:
- tokens: bfloat16 [48, 128, 1024], P('clip', None, 'mp'), may hold values from -6 to 6
- bottleneck: bfloat16 [16, 4, 1024], P('clip', None, 'mp'), may hold values from -6 to 6
- clip_lengths: int32 [16], replicated, may hold values from 2 to 4, as said below
- video_blocks: int32 [16], replicated, may hold values from 1 to 3, as said below
- store_map: int32 [16, 3], replicated, may hold values from -1 to 63, as said below
- norm1_gain: float32 [1024], replicated, may hold values from 0.4 to 1.6
- w_qkv: bfloat16 [3, 1024, 1024], P(None, None, 'mp'), may hold values from -0.625 to 0.625
- w_out: bfloat16 [1024, 1024], P('mp'), may hold values from -0.1875 to 0.1875
- norm2_gain: float32 [1024], replicated, may hold values from 0.4 to 1.6
- w_up: bfloat16 [1024, 4096], P(None, 'mp'), may hold values from -0.1875 to 0.1875
- w_down: bfloat16 [4096, 1024], P('mp'), may hold values from -0.09375 to 0.09375
Outputs:
- mixed_tokens: bfloat16 [48, 128, 1024], P('clip', None, 'mp')
- merged_bottleneck: bfloat16 [16, 4, 1024], P('clip', None, 'mp')
The draws below stay inside these ranges and needn't reach their ends.
Inputs may be any that keep to these rules, and one draw needn't show every extreme that they name: clip_lengths[c] counts the blocks of the clip owned by index c of clip. The first video_blocks[c] blocks of clip c are video, the others up to clip_lengths[c] audio; video_blocks[c] <= clip_lengths[c] - 1. store_map[d, s] = c * 4 + b when slot s of device d along clip holds block b of clip c, and -1 when the slot is empty; each block b < clip_lengths[c] of each clip sits in exactly one slot, on a device of the same aligned group of 4 devices along clip as c; no device holds two blocks of one clip.
All inputs are finite; a program needn't handle non-finite values.
Results may differ from the reference program's by a relative error of at most 0.006.
Values may be sent and summed in bfloat16 or wider, within the bound.
A program may use at most 128 MiB of HBM per device.

```python
import jax
import jax.numpy as jnp
from jax import lax

D = 1024
HEADS = 16
FF = 4096
HEAD_DIM = 64
BLK = 128
NB = 4
SLOT_DEV = 4
STORE_DEV = 3
GROUP = 4
CLIPS = 16


def layout(key):
    groups = CLIPS // GROUP
    base = jax.random.fold_in(key, 11)
    keys = [jax.random.fold_in(base, index) for index in range(5)]
    spots = jnp.arange(GROUP, dtype=jnp.int32)
    first = jax.random.randint(keys[0], (groups, GROUP), 0, 1 << 20) * GROUP + spots
    order = jnp.argsort(first, axis=1).astype(jnp.int32)
    ranking = jnp.argsort(order, axis=1).astype(jnp.int32)
    longer = jax.random.randint(keys[1], (groups, GROUP), SLOT_DEV // 2 + 1, SLOT_DEV + 1)
    shorter = jax.random.randint(keys[2], (groups, GROUP), 2, SLOT_DEV // 2 + 1)
    lengths = jnp.where(ranking % 2 == 0, longer, shorter)
    lengths = jnp.where(ranking == 0, SLOT_DEV, lengths).astype(jnp.int32)
    video = (1 + jax.random.randint(keys[3], (groups, GROUP), 0, 1 << 20) % (lengths - 1)).astype(jnp.int32)
    by_rank = jnp.take_along_axis(lengths, order, axis=1)
    ends = jnp.cumsum(by_rank, axis=1).astype(jnp.int32)
    starts = ends - by_rank
    second = jax.random.randint(keys[4], (groups, GROUP), 0, 1 << 20) * GROUP + spots
    residue = jnp.argsort(jnp.argsort(second, axis=1), axis=1).astype(jnp.int32)
    slots = jnp.arange(STORE_DEV, dtype=jnp.int32)
    position = residue[:, :, None] + GROUP * slots[None, None, :]
    owner_rank = jnp.sum((ends[:, None, None, :] <= position[:, :, :, None]).astype(jnp.int32), axis=-1)
    live = owner_rank < GROUP
    safe = jnp.minimum(owner_rank, GROUP - 1).reshape(groups, GROUP * STORE_DEV)
    start_of = jnp.take_along_axis(starts, safe, axis=1).reshape(groups, GROUP, STORE_DEV)
    owner_spot = jnp.take_along_axis(order, safe, axis=1).reshape(groups, GROUP, STORE_DEV)
    owner = owner_spot + GROUP * jnp.arange(groups, dtype=jnp.int32)[:, None, None]
    entry = jnp.where(live, owner * SLOT_DEV + position - start_of, -1).astype(jnp.int32)
    return (lengths.reshape(CLIPS), video.reshape(CLIPS), entry.reshape(CLIPS, STORE_DEV))


def draw_clip_lengths(key, part):
    return layout(key)[0]


def draw_video_blocks(key, part):
    return layout(key)[1]


def draw_store_map(key, part):
    return layout(key)[2]


def draw_w_qkv(key, part):
    raw = jnp.clip(jax.random.normal(jax.random.fold_in(key, 3), (3, D, D), jnp.float32), -4.0, 4.0) * D ** (-0.5)
    return raw.astype(jnp.bfloat16)


def level_of(own_key, extent, cuts, low, high):
    level, own = 1.0, jax.random.fold_in(own_key, 6)
    for dim, shards_of in cuts:
        draws = jnp.exp(jax.random.uniform(jax.random.fold_in(own, dim), (shards_of,), jnp.float32, low / len(cuts), high / len(cuts)))
        level = level * jnp.repeat(draws, extent[dim] // shards_of).reshape([-1 if axis == dim else 1 for axis in range(len(extent))])
    return level


def gaussian(key, shape, deviation, most, shards=(), kind=jnp.bfloat16):
    drawn = deviation * jax.random.normal(key, shape, jnp.float32)
    if shards:
        drawn = drawn * level_of(key, shape, shards, -0.22, 0.18)
    return jnp.clip(drawn, -most, most).astype(kind)


def setup_inputs(seed: int = 0) -> dict:
    seeds = jax.random.split(jax.random.key(seed), 12)
    tokens = gaussian(seeds[0], (CLIPS * STORE_DEV, BLK, D), 1.0, 6.0, ((0, 16), (2, 2)))
    bottleneck = gaussian(seeds[1], (CLIPS, NB, D), 1.0, 6.0, ((0, 16), (2, 2)))
    clip_lengths = draw_clip_lengths(jax.random.fold_in(seeds[11], 71), 0)
    video_blocks = draw_video_blocks(jax.random.fold_in(seeds[11], 71), 0)
    store_map = draw_store_map(jax.random.fold_in(seeds[11], 71), 0)
    norm1_gain = jnp.clip(1.0 + 0.12 * jax.random.normal(seeds[5], (D,), jnp.float32), 0.4, 1.6)
    w_qkv = draw_w_qkv(jax.random.fold_in(seeds[11], 71), 0)
    w_out = gaussian(seeds[7], (D, D), D ** -0.5, 0.1875, ((0, 2),))
    norm2_gain = jnp.clip(1.0 + 0.12 * jax.random.normal(seeds[8], (D,), jnp.float32), 0.4, 1.6)
    w_up = gaussian(seeds[9], (D, FF), D ** -0.5, 0.1875, ((1, 2),))
    w_down = gaussian(seeds[10], (FF, D), FF ** -0.5, 0.09375, ((0, 2),))
    return {"tokens": tokens, "bottleneck": bottleneck, "clip_lengths": clip_lengths, "video_blocks": video_blocks, "store_map": store_map, "norm1_gain": norm1_gain, "w_qkv": w_qkv, "w_out": w_out, "norm2_gain": norm2_gain, "w_up": w_up, "w_down": w_down}


def layer_norm(rows, gain):
    mean = lax.optimization_barrier(jnp.mean(rows, axis=-1, keepdims=True))
    centred = rows - mean
    moment = lax.optimization_barrier(jnp.mean(centred * centred, axis=-1, keepdims=True))
    return centred * lax.rsqrt(moment + 1e-05) * gain.astype(jnp.float32)

def attend(scores, allowed, values):
    masked = jnp.where(allowed, scores, -1e+30)
    top = lax.optimization_barrier(jnp.max(masked, axis=-1, keepdims=True))
    weights = jnp.where(allowed, jnp.exp(masked - top), 0.0)
    weights = (weights / lax.optimization_barrier(jnp.sum(weights, axis=-1, keepdims=True))).astype(jnp.bfloat16)
    return jnp.dot(weights, values, preferred_element_type=jnp.float32)

def reference(tokens, bottleneck, clip_lengths, video_blocks, store_map, norm1_gain, w_qkv, w_out, norm2_gain, w_up, w_down):
    total_rows = SLOT_DEV * BLK
    flat_map = store_map.reshape(-1).astype(jnp.int32)
    target = jnp.where(flat_map >= 0, flat_map, CLIPS * SLOT_DEV).astype(jnp.int32)
    placed = jnp.zeros((CLIPS * SLOT_DEV, BLK, D), tokens.dtype).at[target].set(tokens, mode='drop')
    placed = placed.reshape(CLIPS, total_rows, D)

    def one_clip(items):
        clip_rows, extra, length, video = items
        rows = jnp.concatenate([clip_rows, extra], axis=0)
        normed = layer_norm(rows.astype(jnp.float32), norm1_gain).astype(jnp.bfloat16)
        query = jnp.dot(normed, w_qkv[0], preferred_element_type=jnp.float32).astype(jnp.bfloat16)
        keys = jnp.dot(normed, w_qkv[1], preferred_element_type=jnp.float32).astype(jnp.bfloat16)
        values = jnp.dot(normed, w_qkv[2], preferred_element_type=jnp.float32).astype(jnp.bfloat16)
        block_of = jnp.arange(total_rows, dtype=jnp.int32) // BLK
        token_mode = jnp.where(block_of < video, 0, jnp.where(block_of < length, 1, -1)).astype(jnp.int32)
        key_mode = jnp.concatenate([token_mode, jnp.full((NB,), 2, jnp.int32)])
        token_allow = (key_mode[None, :] == token_mode[:, None]) | (key_mode[None, :] == 2)
        video_allow = jnp.broadcast_to((key_mode == 0) | (key_mode == 2), (NB, total_rows + NB))
        audio_allow = jnp.broadcast_to((key_mode == 1) | (key_mode == 2), (NB, total_rows + NB))
        pieces = []
        for head in range(HEADS):
            cols = slice(head * HEAD_DIM, (head + 1) * HEAD_DIM)
            scores = lax.dot_general(query[:, cols], keys[:, cols], (((1,), (1,)), ((), ())), preferred_element_type=jnp.float32)
            scores = scores * HEAD_DIM ** (-0.5)
            own = attend(scores[:total_rows], token_allow, values[:, cols])
            seen_video = attend(scores[total_rows:], video_allow, values[:, cols])
            seen_audio = attend(scores[total_rows:], audio_allow, values[:, cols])
            pieces.append(jnp.concatenate([own, 0.5 * (seen_video + seen_audio)], axis=0))
        context = jnp.concatenate(pieces, axis=1).astype(jnp.bfloat16)
        after = (rows.astype(jnp.float32) + jnp.dot(context, w_out, preferred_element_type=jnp.float32)).astype(jnp.bfloat16)
        normed2 = layer_norm(after.astype(jnp.float32), norm2_gain).astype(jnp.bfloat16)
        active = jax.nn.gelu(jnp.dot(normed2, w_up, preferred_element_type=jnp.float32), approximate=True).astype(jnp.bfloat16)
        merged = (after.astype(jnp.float32) + jnp.dot(active, w_down, preferred_element_type=jnp.float32)).astype(jnp.bfloat16)
        return (merged[:total_rows], merged[total_rows:])
    merged_rows, merged_extra = lax.map(one_clip, (placed, bottleneck, clip_lengths, video_blocks))
    merged_rows = merged_rows.reshape(CLIPS * SLOT_DEV, BLK, D)
    picked = merged_rows[jnp.maximum(flat_map, 0)]
    mixed_tokens = jnp.where(flat_map[:, None, None] >= 0, picked, jnp.zeros_like(picked))
    return (mixed_tokens, merged_extra)
```

```python
import functools

import jax
import jax.numpy as jnp
from jax import lax
from jax.experimental import pallas as pl
from jax.experimental.pallas import tpu as pltpu
from jax.sharding import PartitionSpec as P

HEAD_DIM = 64
GROUP = 4
EPS = 1e-05
NEG = -1e30
EXTRA = 16
LOG2E = 1.4426950408889634
GELU = 0.7978845608028654
LOOK = 2
SCOPE = jax.named_scope
BF16 = jnp.bfloat16
F32 = jnp.float32


def layer_norm(halves, gain):
    x = jnp.concatenate([h.astype(F32) for h in halves], axis=1)
    mean = jnp.mean(x, axis=-1, keepdims=True)
    centred = x - mean
    moment = jnp.mean(centred * centred, axis=-1, keepdims=True)
    return (centred * lax.rsqrt(moment + EPS) * gain).astype(BF16)


def dot(a, b):
    return jnp.dot(a, b, preferred_element_type=F32)


def gelu(y):
    rate = y * (0.044715 * GELU * (y * y) + GELU)
    half = 0.5 * y
    return half + half * jnp.tanh(rate)


def kernel(
    blk,
    nb,
    video_hbm,
    map_hbm,
    tok_hbm,
    bot_hbm,
    g1_hbm,
    g2_hbm,
    wqkv_hbm,
    wout_hbm,
    wup_hbm,
    wdown_hbm,
    out_ref,
    outb_ref,
    video_ref,
    map_ref,
    bot_ref,
    g1_ref,
    g2_ref,
    tok,
    wqkv,
    wout,
    wup,
    wdown,
    snd,
    x,
    ext,
    qm,
    qb,
    k,
    vt,
    ctx,
    ps1,
    pr1,
    own1,
    aft,
    act,
    ps2,
    pr2,
    own2,
    fin,
    ret,
    ld_sem,
    send_sem,
    recv_sem,
):
    slots = tok.shape[0]
    width = tok.shape[2]
    pairs = vt.shape[0]
    keys = vt.shape[2]
    rows = x.shape[1]
    ff = wdown.shape[1]
    total = GROUP * blk

    me = lax.axis_index("clip")
    core = lax.axis_index("mp")
    peer = 1 - core
    bit0 = lax.rem(me, 2)
    bit1 = lax.rem(lax.div(me, 2), 2)
    flip0 = 1 - 2 * bit0
    flip1 = 2 - 4 * bit1
    partner = [me, me + flip0, me + flip1, me + flip0 + flip1]

    barrier = pltpu.get_barrier_semaphore()
    for r in range(1, GROUP):
        pl.semaphore_signal(barrier, inc=1, device_id={"clip": partner[r]})
    pl.semaphore_signal(barrier, inc=1, device_id={"mp": peer})

    def load(i, src, dst):
        return pltpu.make_async_copy(src, dst, ld_sem.at[i])

    halves = [pl.ds(h * width, width) for h in range(2)]
    first = [
        load(0, tok_hbm, tok),
        load(1, map_hbm, map_ref),
        load(2, video_hbm, video_ref),
        load(3, bot_hbm, bot_ref),
        load(4, g1_hbm, g1_ref),
        load(5, g2_hbm, g2_ref),
    ]
    load_qkv = load(6, wqkv_hbm, wqkv)
    tiles = wup.shape[0]
    load_out = [load(7 + h, wout_hbm.at[:, halves[h]], wout.at[h]) for h in range(2)]
    load_down = [load(9 + h, wdown_hbm.at[:, halves[h]], wdown.at[h]) for h in range(2)]
    load_up = [load(11 + t, wup_hbm.at[:, pl.ds(t * width, width)], wup.at[t]) for t in range(tiles)]
    for c in first:
        c.start()

    column = lax.broadcasted_iota(jnp.int32, (1, width), 1)
    low = lax.rem(column, 2 * HEAD_DIM) < HEAD_DIM
    for j in range(pairs):
        vt[j, 2 * HEAD_DIM :] = jnp.ones((EXTRA, keys), BF16)

    for c in first:
        c.wait()
    for c in (load_qkv, *load_out, *load_up, *load_down):
        c.start()

    entry = [map_ref[s, me] for s in range(slots)]
    own = [jnp.where(e >= 0, lax.div(e, GROUP), -1) for e in entry]
    pick = []
    for r in range(GROUP):
        chosen = jnp.int32(0)
        for s in range(slots):
            chosen = jnp.where(own[s] == partner[r], s, chosen)
        pick.append(chosen)
    video = video_ref[me]
    mode = []
    for r in range(GROUP):
        m = jnp.int32(-1)
        for s in range(slots):
            e = map_ref[s, partner[r]]
            mine = (e >= 0) & (lax.div(e, GROUP) == me)
            m = jnp.where(mine, jnp.where(lax.rem(e, GROUP) < video, 0, 1), m)
        mode.append(m)

    order = [1, 2, 3, 0]
    place = [(GROUP - 1) * blk] + [(r - 1) * blk for r in range(1, GROUP)]
    span = [pl.ds(place[0], blk + EXTRA)] + [pl.ds(place[r], blk) for r in range(1, GROUP)]

    def ici(r, src, dst, base):
        return pltpu.make_async_remote_copy(
            src_ref=src,
            dst_ref=dst,
            send_sem=send_sem.at[base + r],
            recv_sem=recv_sem.at[base + r],
            device_id={"clip": partner[r]},
        )

    def d2d(r, src, dst, base):
        return pltpu.make_async_remote_copy(
            src_ref=src,
            dst_ref=dst,
            send_sem=send_sem.at[base + r],
            recv_sem=recv_sem.at[base + r],
            device_id={"mp": peer},
        )

    half = x.at[core]
    arrive = [ici(r, snd.at[r - 1], half.at[span[r]], 0) if r else None for r in range(GROUP)]
    share = [d2d(r, half.at[span[r]], half.at[span[r]], 4) for r in range(GROUP)]
    proj = [d2d(r, ps1.at[:, span[r]], pr1.at[:, span[r]], 8) for r in range(GROUP)]
    down = [d2d(r, ps2.at[span[r]], pr2.at[span[r]], 12) for r in range(GROUP)]
    back = [ici(r, fin.at[r - 1], ret.at[r], 16) if r else None for r in range(GROUP)]

    for r in range(1, GROUP):
        snd[r - 1] = tok[pick[r]]
    x[core, pl.ds(place[0], blk)] = tok[pick[0]]
    small = bot_ref[0].astype(F32)
    for i in range(EXTRA // nb):
        ext[pl.ds(i * nb, nb)] = small
    x[core, pl.ds(total, EXTRA)] = ext[...].astype(BF16)

    with SCOPE("barrier"):
        pl.semaphore_wait(barrier, GROUP)
    for r in (1, 2, 3):
        arrive[r].start()
    share[0].start()

    def seen(m, s):
        return jnp.where((mode[s] == m) & (mode[s] >= 0), 0.0, NEG).astype(F32)

    tail = lax.broadcasted_iota(jnp.int32, (EXTRA, 1), 0) < nb

    def project(r):
        n = layer_norm([x[0, span[r]], x[1, span[r]]], g1_ref[...])
        y = dot(n, wqkv[0]) * (HEAD_DIM ** (-0.5) * LOG2E)
        y0 = jnp.where(low, y, 0.0).astype(BF16)
        y1 = jnp.where(low, 0.0, y).astype(BF16)
        qm[0, span[r]] = y0
        qm[1, span[r]] = y1
        if r == 0:
            e = y[blk:]
            head = lax.div(column, HEAD_DIM)
            for h in range(2 * pairs):
                qb[pl.ds(h * EXTRA, EXTRA)] = jnp.where(head == h, e, 0.0).astype(BF16)
        k[span[r]] = dot(n, wqkv[1]).astype(BF16)
        y = dot(n, wqkv[2])
        for j in range(pairs):
            cols = y[:, j * 128 : (j + 1) * 128]
            vt[j, :128, pl.ds(place[r], blk)] = cols[:blk].T.astype(BF16)
            if r == 0:
                padded = jnp.concatenate([cols[blk:], jnp.zeros((128 - EXTRA, 128), F32)], axis=0)
                vt[j, :128, pl.ds(total, 128)] = padded.T.astype(BF16)

    def soften(s, bias):
        n = s.shape[1]
        parts = [s[p * blk : (p + 1) * blk] for p in range(GROUP)]
        last = jnp.where(tail, s[total:], NEG)
        tops = [jnp.max(p.reshape(blk // 8, 8, n), axis=0) + b for p, b in zip(parts, bias)]
        tops.append(jnp.max(last.reshape(EXTRA // 8, 8, n), axis=0))
        top = tops[0]
        for t in tops[1:]:
            top = jnp.maximum(top, t)
        top = jnp.max(top, axis=0, keepdims=True)
        p = [jnp.exp2(q + (b - top)).astype(BF16) for q, b in zip(parts, bias)]
        p.append(jnp.exp2(last - top).astype(BF16))
        p.append(jnp.zeros((keys - rows, n), BF16))
        return jnp.concatenate(p, axis=0)

    def scores(a, b):
        return lax.dot_general(a, b, (((1,), (1,)), ((), ())), preferred_element_type=F32)

    def score(item):
        r, j = item
        if r is None:
            return scores(k[...], qb[...])
        at = pl.ds(place[r], blk)
        cols = slice(j * 128, (j + 1) * 128)
        both = jnp.concatenate([qm[0, at, cols], qm[1, at, cols]], axis=0)
        return scores(k[:, cols], both)

    def mix(item, s):
        r, j = item
        if r is None:
            mix_small(s)
            return
        at = pl.ds(place[r], blk)
        cols = slice(j * 128, (j + 1) * 128)
        p = soften(s, [seen(mode[r], b) for b in order])
        o = dot(vt[j], p)
        under = 1.0 / o[128:129]
        d = HEAD_DIM
        o = jnp.concatenate([o[:d, :blk] * under[:, :blk], o[d : 2 * d, blk:] * under[:, blk:]], axis=0)
        ctx[at, cols] = o.T.astype(BF16)

    def mix_small(s):
        n = 2 * pairs * EXTRA
        step = lax.rem(lax.broadcasted_iota(jnp.int32, (1, n), 1), EXTRA)
        audio = (step >= nb) & (step < 2 * nb)
        p = soften(s, [jnp.where(audio, seen(1, b), seen(0, b)) for b in order])
        for j in range(pairs):
            o = dot(vt[j], p)
            o = (o[:128] * (1.0 / o[128:129])).T
            at = 2 * j * EXTRA
            e = jnp.where(low[:, :128], o[at : at + EXTRA], o[at + EXTRA : at + 2 * EXTRA])
            e = 0.5 * (e + pltpu.roll(e, EXTRA - nb, 0))
            ctx[pl.ds(total, EXTRA), j * 128 : (j + 1) * 128] = e.astype(BF16)

    def project_out(r):
        c = ctx[span[r]]
        for h in range(2):
            y = dot(c, wout[h])
            ps1[h, span[r]] = y.astype(BF16)
            own1[h, span[r]] = y
        proj[r].start()

    def normed_after(r):
        at = span[r]
        parts = []
        for h in range(2):
            t = x[h, at].astype(F32) + (own1[h, at] + pr1[h, at].astype(F32))
            t = t.astype(BF16)
            aft[h, at] = t
            parts.append(t)
        return layer_norm(parts, g2_ref[...])

    def grow(r, n):
        for t in range(tiles):
            act[span[r], t * width : (t + 1) * width] = gelu(dot(n, wup[t])).astype(BF16)

    def shrink(r):
        a = act[span[r]]
        ps2[span[r]] = dot(a, wdown[peer]).astype(BF16)
        down[r].start()
        own2[span[r]] = dot(a, wdown[core])

    def finish(r):
        at = span[r]
        merged = aft[core, at].astype(F32) + (own2[at] + pr2[at].astype(F32))
        if r == 0:
            ret[0] = merged[:blk].astype(BF16)
            outb_ref[0] = merged[blk : blk + nb].astype(BF16)
        else:
            fin[r - 1] = merged.astype(BF16)
            back[r].start()

    with SCOPE("w0"):
        load_qkv.wait()
        share[0].wait_recv()
    with SCOPE("project0"):
        project(0)
    for r in (1, 2):
        with SCOPE("arr%d" % r):
            arrive[r].wait_recv()
        share[r].start()
    for r in (1, 2):
        with SCOPE("sh%d" % r):
            share[r].wait_recv()
        with SCOPE("project%d" % r):
            project(r)
    with SCOPE("arr3"):
        arrive[3].wait_recv()
    share[3].start()
    with SCOPE("ldwait"):
        for c in (*load_out, *load_up, *load_down):
            c.wait()
    with SCOPE("sh3"):
        share[3].wait_recv()
    items = [(r, j) for r in (3, 1, 2, 0) for j in range(pairs)]
    items.insert(3 * pairs, (None, 0))
    emit_out = {(1, 1): 3, (2, 1): 1, (0, 1): 2}
    with SCOPE("attention"):
        project(3)
        waiting = {}
        for t in range(len(items) + LOOK):
            if t < len(items):
                waiting[t] = score(items[t])
            if t >= LOOK:
                mix(items[t - LOOK], waiting.pop(t - LOOK))
                if items[t - LOOK] in emit_out:
                    project_out(emit_out[items[t - LOOK]])
        project_out(0)
    with SCOPE("wproj31"):
        proj[3].wait_recv()
        proj[1].wait_recv()
    with SCOPE("ffnA"):
        grow(3, normed_after(3))
        n = normed_after(1)
        shrink(3)
        grow(1, n)
    with SCOPE("wB"):
        proj[2].wait_recv()
        down[3].wait_recv()
    with SCOPE("ffnB"):
        finish(3)
        n = normed_after(2)
        shrink(1)
        grow(2, n)
    with SCOPE("wC"):
        proj[0].wait_recv()
        down[1].wait_recv()
    with SCOPE("ffnC"):
        finish(1)
        n = normed_after(0)
        shrink(2)
        grow(0, n)
    with SCOPE("wD"):
        down[2].wait_recv()
    with SCOPE("ffnD"):
        finish(2)
        shrink(0)
    with SCOPE("wE"):
        down[0].wait_recv()
    with SCOPE("fin0"):
        finish(0)
    with SCOPE("backwait"):
        for r in (3, 1, 2):
            back[r].wait_recv()
    for s in range(slots):
        where = jnp.int32(0)
        for r in range(GROUP):
            where = jnp.where(own[s] == partner[r], r, where)
        live = jnp.where(entry[s] >= 0, 1.0, 0.0).astype(F32)
        block = ret[where].astype(F32)
        out_ref[s] = (block * live).astype(BF16)
    for r in range(1, GROUP):
        arrive[r].wait_send()
        back[r].wait_send()
    for r in range(GROUP):
        for c in (share, proj, down):
            c[r].wait_send()


def place(stored_ref, merged_ref, out_ref, outb_ref):
    out_ref[...] = stored_ref[...]
    outb_ref[...] = merged_ref[...]


def body(
    tokens,
    bottleneck,
    clip_lengths,
    video_blocks,
    store_map,
    norm1_gain,
    w_qkv,
    w_out,
    norm2_gain,
    w_up,
    w_down,
):
    slots, blk, width = tokens.shape
    nb = bottleneck.shape[1]
    dim = w_qkv.shape[1]
    inner = w_qkv.shape[2]
    ff = w_up.shape[1]
    pairs = inner // 128
    rows = GROUP * blk + EXTRA
    keys = (rows + 127) // 128 * 128
    vmem = pl.BlockSpec(memory_space=pltpu.VMEM)
    hbm = pl.BlockSpec(memory_space=pltpu.HBM)
    V = pltpu.VMEM
    stored, merged = pl.pallas_call(
        functools.partial(kernel, blk, nb),
        out_shape=(
            jax.ShapeDtypeStruct(tokens.shape, BF16),
            jax.ShapeDtypeStruct(bottleneck.shape, BF16),
        ),
        in_specs=[hbm] * 10,
        out_specs=(vmem, vmem),
        scratch_shapes=[
            pltpu.SMEM(video_blocks.shape, jnp.int32),
            pltpu.SMEM(store_map.shape[::-1], jnp.int32),
            V(bottleneck.shape, BF16),
            V((1, dim), F32),
            V((1, dim), F32),
            V((slots, blk, width), BF16),
            V(w_qkv.shape, BF16),
            V((2, inner, width), BF16),
            V((ff // width, dim, width), BF16),
            V((2, ff, width), BF16),
            V((GROUP - 1, blk, width), BF16),
            V((2, rows, width), BF16),
            V((EXTRA, width), F32),
            V((2, rows, inner), BF16),
            V((2 * pairs * EXTRA, inner), BF16),
            V((rows, inner), BF16),
            V((pairs, 128 + EXTRA, keys), BF16),
            V((rows, inner), BF16),
            V((2, rows, width), BF16),
            V((2, rows, width), BF16),
            V((2, rows, width), F32),
            V((2, rows, width), BF16),
            V((rows, ff), BF16),
            V((rows, width), BF16),
            V((rows, width), BF16),
            V((rows, width), F32),
            V((GROUP - 1, blk, width), BF16),
            V((GROUP, blk, width), BF16),
            pltpu.SemaphoreType.DMA((11 + ff // width,)),
            pltpu.SemaphoreType.DMA((20,)),
            pltpu.SemaphoreType.DMA((20,)),
        ],
        compiler_params=pltpu.CompilerParams(collective_id=0, has_side_effects=True, vmem_limit_bytes=40 << 20),
        name="merge_layer",
    )(
        *(
            pltpu.with_memory_space_constraint(a, pltpu.HBM)
            for a in (
                video_blocks,
                store_map.T,
                tokens,
                bottleneck,
                norm1_gain.reshape(1, dim),
                norm2_gain.reshape(1, dim),
                w_qkv,
                w_out,
                w_up,
                w_down,
            )
        )
    )
    return pl.pallas_call(
        place,
        out_shape=(
            jax.ShapeDtypeStruct(tokens.shape, BF16),
            jax.ShapeDtypeStruct(bottleneck.shape, BF16),
        ),
        in_specs=[vmem, vmem],
        out_specs=(vmem, vmem),
        compiler_params=pltpu.CompilerParams(vmem_limit_bytes=4 << 20),
        name="place",
    )(stored, merged)


def solution(mesh):
    placed = (
        P("clip", None, "mp"),
        P("clip", None, "mp"),
        P(),
        P(),
        P(),
        P(),
        P(None, None, "mp"),
        P("mp", None),
        P(),
        P(None, "mp"),
        P("mp", None),
    )
    return jax.shard_map(
        body,
        mesh=mesh,
        in_specs=placed,
        out_specs=(P("clip", None, "mp"), P("clip", None, "mp")),
        check_vma=False,
    )
```

```python
import functools

import jax
import jax.numpy as jnp
from jax import lax
from jax.experimental import pallas as pl
from jax.experimental.pallas import tpu as pltpu
from jax.sharding import PartitionSpec as P

HEAD_DIM = 64
GROUP = 4
EPS = 1e-05
NEG = -1e30
EXTRA = 16
LOG2E = 1.4426950408889634
GELU = 0.7978845608028654
LOOK = 2
SCOPE = jax.named_scope
BF16 = jnp.bfloat16
F32 = jnp.float32


def layer_norm(halves, gain):
    x = jnp.concatenate([h.astype(F32) for h in halves], axis=1)
    mean = jnp.mean(x, axis=-1, keepdims=True)
    centred = x - mean
    moment = jnp.mean(centred * centred, axis=-1, keepdims=True)
    return (centred * lax.rsqrt(moment + EPS) * gain).astype(BF16)


def dot(a, b):
    return jnp.dot(a, b, preferred_element_type=F32)


def gelu(y):
    rate = y * (0.044715 * GELU * (y * y) + GELU)
    half = 0.5 * y
    return half + half * jnp.tanh(rate)


def kernel(
    blk,
    nb,
    video_hbm,
    map_hbm,
    tok_hbm,
    bot_hbm,
    g1_hbm,
    g2_hbm,
    wqkv_hbm,
    wout_hbm,
    wup_hbm,
    wdown_hbm,
    out_ref,
    outb_ref,
    video_ref,
    map_ref,
    bot_ref,
    g1_ref,
    g2_ref,
    tok,
    wqkv,
    wout,
    wup,
    wdown,
    snd,
    x,
    ext,
    qm,
    qb,
    k,
    vt,
    part,
    part_top,
    ctx,
    ps1,
    pr1,
    own1,
    aft,
    act,
    ps2,
    pr2,
    own2,
    fin,
    ret,
    ld_sem,
    send_sem,
    recv_sem,
):
    slots = tok.shape[0]
    width = tok.shape[2]
    pairs = vt.shape[0]
    keys = vt.shape[2]
    rows = x.shape[1]
    ff = wdown.shape[1]

    me = lax.axis_index("clip")
    core = lax.axis_index("mp")
    peer = 1 - core
    bit0 = lax.rem(me, 2)
    bit1 = lax.rem(lax.div(me, 2), 2)
    flip0 = 1 - 2 * bit0
    flip1 = 2 - 4 * bit1
    partner = [me, me + flip0, me + flip1, me + flip0 + flip1]

    barrier = pltpu.get_barrier_semaphore()
    for r in range(1, GROUP):
        pl.semaphore_signal(barrier, inc=1, device_id={"clip": partner[r]})
    pl.semaphore_signal(barrier, inc=1, device_id={"mp": peer})

    def load(i, src, dst):
        return pltpu.make_async_copy(src, dst, ld_sem.at[i])

    halves = [pl.ds(h * width, width) for h in range(2)]
    first = [
        load(0, tok_hbm, tok),
        load(1, map_hbm, map_ref),
        load(2, video_hbm, video_ref),
        load(3, bot_hbm, bot_ref),
        load(4, g1_hbm, g1_ref),
        load(5, g2_hbm, g2_ref),
    ]
    load_qkv = load(6, wqkv_hbm, wqkv)
    tiles = wup.shape[0]
    load_out = [load(7 + h, wout_hbm.at[:, halves[h]], wout.at[h]) for h in range(2)]
    load_down = [load(9 + h, wdown_hbm.at[:, halves[h]], wdown.at[h]) for h in range(2)]
    load_up = [load(11 + t, wup_hbm.at[:, pl.ds(t * width, width)], wup.at[t]) for t in range(tiles)]
    for c in first:
        c.start()

    column = lax.broadcasted_iota(jnp.int32, (1, width), 1)
    low = lax.rem(column, 2 * HEAD_DIM) < HEAD_DIM
    for j in range(pairs):
        vt[j, 2 * HEAD_DIM :] = jnp.ones((EXTRA, keys), BF16)

    for c in first:
        c.wait()
    for c in (load_qkv, *load_out, *load_up, *load_down):
        c.start()

    entry = [map_ref[s, me] for s in range(slots)]
    own = [jnp.where(e >= 0, lax.div(e, GROUP), -1) for e in entry]
    pick = []
    for r in range(GROUP):
        chosen = jnp.int32(0)
        for s in range(slots):
            chosen = jnp.where(own[s] == partner[r], s, chosen)
        pick.append(chosen)
    video = video_ref[me]
    mode = []
    for r in range(GROUP):
        m = jnp.int32(-1)
        for s in range(slots):
            e = map_ref[s, partner[r]]
            mine = (e >= 0) & (lax.div(e, GROUP) == me)
            m = jnp.where(mine, jnp.where(lax.rem(e, GROUP) < video, 0, 1), m)
        mode.append(m)

    order = [1, 2, 0]
    total = (GROUP - 1) * blk
    late = total + EXTRA
    place = [2 * blk, 0, blk, late]
    lanes = [2 * blk, 0, blk, total + 128]
    span = [pl.ds(place[0], blk + EXTRA)] + [pl.ds(place[r], blk) for r in range(1, GROUP)]

    def ici(r, src, dst, base):
        return pltpu.make_async_remote_copy(
            src_ref=src,
            dst_ref=dst,
            send_sem=send_sem.at[base + r],
            recv_sem=recv_sem.at[base + r],
            device_id={"clip": partner[r]},
        )

    def d2d(r, src, dst, base):
        return pltpu.make_async_remote_copy(
            src_ref=src,
            dst_ref=dst,
            send_sem=send_sem.at[base + r],
            recv_sem=recv_sem.at[base + r],
            device_id={"mp": peer},
        )

    half = x.at[core]
    arrive = [ici(r, snd.at[r - 1], half.at[span[r]], 0) if r else None for r in range(GROUP)]
    share = [d2d(r, half.at[span[r]], half.at[span[r]], 4) for r in range(GROUP)]
    proj = [d2d(r, ps1.at[:, span[r]], pr1.at[:, span[r]], 8) for r in range(GROUP)]
    down = [d2d(r, ps2.at[span[r]], pr2.at[span[r]], 12) for r in range(GROUP)]
    back = [ici(r, fin.at[r - 1], ret.at[r], 16) if r else None for r in range(GROUP)]

    for r in range(1, GROUP):
        snd[r - 1] = tok[pick[r]]
    x[core, pl.ds(place[0], blk)] = tok[pick[0]]
    small = bot_ref[0].astype(F32)
    for i in range(EXTRA // nb):
        ext[pl.ds(i * nb, nb)] = small
    x[core, pl.ds(total, EXTRA)] = ext[...].astype(BF16)

    with SCOPE("barrier"):
        pl.semaphore_wait(barrier, GROUP)
    for r in (1, 2, 3):
        arrive[r].start()
    share[0].start()

    def seen(m, s):
        return jnp.where((mode[s] == m) & (mode[s] >= 0), 0.0, NEG).astype(F32)

    tail = lax.broadcasted_iota(jnp.int32, (EXTRA, 1), 0) < nb

    def norm(r):
        return layer_norm([x[0, span[r]], x[1, span[r]]], g1_ref[...])

    def project(r, n, then=None):
        y = dot(n, wqkv[0]) * (HEAD_DIM ** (-0.5) * LOG2E)
        y0 = jnp.where(low, y, 0.0).astype(BF16)
        y1 = jnp.where(low, 0.0, y).astype(BF16)
        qm[0, span[r]] = y0
        qm[1, span[r]] = y1
        if r == 0:
            e = y[blk:]
            head = lax.div(column, HEAD_DIM)
            for h in range(2 * pairs):
                qb[pl.ds(h * EXTRA, EXTRA)] = jnp.where(head == h, e, 0.0).astype(BF16)
        k[span[r]] = dot(n, wqkv[1]).astype(BF16)
        if then is not None:
            then()
        y = dot(n, wqkv[2])
        for j in range(pairs):
            cols = y[:, j * 128 : (j + 1) * 128]
            vt[j, :128, pl.ds(lanes[r], blk)] = cols[:blk].T.astype(BF16)
            if r == 0:
                padded = jnp.concatenate([cols[blk:], jnp.zeros((128 - EXTRA, 128), F32)], axis=0)
                vt[j, :128, pl.ds(total, 128)] = padded.T.astype(BF16)

    def column_max(s):
        m, n = s.shape
        return jnp.max(s.reshape(m // 8, 8, n), axis=0)

    def soften(s, bias, last=None, last_bias=None):
        n = s.shape[1]
        parts = [s[p * blk : (p + 1) * blk] for p in range(GROUP - 1)]
        extra = jnp.where(tail, s[total:late], NEG)
        top = column_max(extra)
        for q, b in zip(parts, bias):
            top = jnp.maximum(top, column_max(q) + b)
        if last is not None:
            top = jnp.maximum(top, column_max(last) + last_bias)
        top = jnp.max(top, axis=0, keepdims=True)
        p = [jnp.exp2(q + (b - top)).astype(BF16) for q, b in zip(parts, bias)]
        p.append(jnp.exp2(extra - top).astype(BF16))
        p.append(jnp.zeros((128 - EXTRA, n), BF16))
        if last is not None:
            p.append(jnp.exp2(last + (last_bias - top)).astype(BF16))
        return jnp.concatenate(p, axis=0), top

    def merge(last, bias, o, top, v):
        best = jnp.maximum(top, jnp.max(column_max(last), axis=0, keepdims=True) + bias)
        p = jnp.exp2(last + (bias - best)).astype(BF16)
        scale = jnp.exp2(top - best)
        return o * scale + dot(v, p)

    def scores(a, b):
        return lax.dot_general(a, b, (((1,), (1,)), ((), ())), preferred_element_type=F32)

    def queries(r, j):
        at = pl.ds(place[r], blk)
        cols = slice(j * 128, (j + 1) * 128)
        return jnp.concatenate([qm[0, at, cols], qm[1, at, cols]], axis=0)

    early = pl.ds(0, late)
    split = total + 128
    step = lax.rem(lax.broadcasted_iota(jnp.int32, (1, 2 * pairs * EXTRA), 1), EXTRA)
    audio = (step >= nb) & (step < 2 * nb)

    def seen_small(b):
        return jnp.where(audio, seen(1, b), seen(0, b))

    def store(r, j, o):
        under = 1.0 / o[128:129]
        d = HEAD_DIM
        o = jnp.concatenate([o[:d, :blk] * under[:, :blk], o[d : 2 * d, blk:] * under[:, blk:]], axis=0)
        ctx[pl.ds(place[r], blk), j * 128 : (j + 1) * 128] = o.T.astype(BF16)

    def first_score(item):
        r, j = item
        return scores(k[early, j * 128 : (j + 1) * 128], queries(r, j))

    def first_mix(item, s):
        r, j = item
        p, top = soften(s, [seen(mode[r], b) for b in order])
        part_top[r - 1, j] = top
        part[r - 1, j] = dot(vt[j, :, :split], p)

    def last_score(item):
        r, j = item
        if r is None:
            return scores(k[early], qb[...]), scores(k[span[3]], qb[...])
        cols = slice(j * 128, (j + 1) * 128)
        q = queries(r, j)
        last = scores(k[span[3], cols], q)
        return (scores(k[early, cols], q), last) if r in (0, 3) else last

    def last_mix(item, s):
        r, j = item
        if r is None:
            p, _ = soften(s[0], [seen_small(b) for b in order], s[1], seen_small(3))
            o = [dot(vt[i], p) for i in range(pairs)]
            for i in range(pairs):
                t = (o[i][:128] * (1.0 / o[i][128:129])).T
                at = 2 * i * EXTRA
                e = jnp.where(low[:, :128], t[at : at + EXTRA], t[at + EXTRA : at + 2 * EXTRA])
                e = 0.5 * (e + pltpu.roll(e, EXTRA - nb, 0))
                ctx[pl.ds(total, EXTRA), i * 128 : (i + 1) * 128] = e.astype(BF16)
        elif r in (0, 3):
            p, _ = soften(s[0], [seen(mode[r], b) for b in order], s[1], seen(mode[r], 3))
            store(r, j, dot(vt[j], p))
        else:
            store(r, j, merge(s, seen(mode[r], 3), part[r - 1, j], part_top[r - 1, j], vt[j, :, split:]))

    def stream(items, score, mix, look, ahead=()):
        waiting = dict(enumerate(ahead))
        for t in range(len(items) + look):
            if len(ahead) <= t < len(items):
                waiting[t] = score(items[t])
            if t >= look:
                mix(items[t - look], waiting.pop(t - look))

    def project_out(r):
        c = ctx[span[r]]
        for h in range(2):
            y = dot(c, wout[h])
            ps1[h, span[r]] = y.astype(BF16)
            own1[h, span[r]] = y

    def normed_after(r):
        at = span[r]
        parts = []
        for h in range(2):
            t = x[h, at].astype(F32) + (own1[h, at] + pr1[h, at].astype(F32))
            t = t.astype(BF16)
            aft[h, at] = t
            parts.append(t)
        return layer_norm(parts, g2_ref[...])

    def grow(r, n):
        for t in range(tiles):
            act[span[r], t * width : (t + 1) * width] = gelu(dot(n, wup[t])).astype(BF16)

    def shrink_peer(r):
        ps2[span[r]] = dot(act[span[r]], wdown[peer]).astype(BF16)

    def shrink_own(r):
        own2[span[r]] = dot(act[span[r]], wdown[core])

    def finish(r):
        at = span[r]
        merged = aft[core, at].astype(F32) + (own2[at] + pr2[at].astype(F32))
        if r == 0:
            ret[0] = merged[:blk].astype(BF16)
            outb_ref[0] = merged[blk : blk + nb].astype(BF16)
        else:
            fin[r - 1] = merged.astype(BF16)
            back[r].start()

    with SCOPE("w0"):
        load_qkv.wait()
        share[0].wait_recv()
    with SCOPE("project0"):
        project(0, norm(0))
    for r in (1, 2):
        with SCOPE("arr%d" % r):
            arrive[r].wait_recv()
        share[r].start()

    def pass_on():
        arrive[3].wait_recv()
        share[3].start()

    pl.when(core == 1)(pass_on)
    for r in (1, 2):
        with SCOPE("sh%d" % r):
            share[r].wait_recv()
    soon = [(r, j) for r in (1, 2) for j in range(pairs)]
    with SCOPE("early"):
        n1 = norm(1)
        n2 = norm(2)
        project(1, n1)
        project(2, n2)
        stream(soon, first_score, first_mix, LOOK)
    with SCOPE("arr3"):
        pl.when(core == 0)(pass_on)
    with SCOPE("ldwait"):
        for c in (*load_out, *load_up, *load_down):
            c.wait()
    with SCOPE("sh3"):
        share[3].wait_recv()
    with SCOPE("late3"):
        mine = [(3, j) for j in range(pairs)]
        ahead = []
        project(3, norm(3), lambda: ahead.extend(last_score(i) for i in mine[:LOOK]))
        stream(mine, last_score, last_mix, LOOK, ahead)
        project_out(3)
    proj[3].start()
    with SCOPE("late12"):
        stream(soon + [(None, 0)], last_score, last_mix, LOOK + 2)
        project_out(1)
    proj[1].start()
    with SCOPE("wproj3"):
        proj[3].wait_recv()
    with SCOPE("ffn3"):
        n = normed_after(3)
        project_out(2)
        grow(3, n)
        shrink_peer(3)
    proj[2].start()
    down[3].start()
    with SCOPE("wproj1"):
        proj[1].wait_recv()
    with SCOPE("ffn1"):
        shrink_own(3)
        grow(1, normed_after(1))
        shrink_peer(1)
    down[1].start()
    with SCOPE("wB"):
        down[3].wait_recv()
    with SCOPE("fin3"):
        finish(3)
    with SCOPE("wC"):
        proj[2].wait_recv()
    with SCOPE("ffn2"):
        shrink_own(1)
        grow(2, normed_after(2))
        shrink_peer(2)
    down[2].start()
    with SCOPE("wC1"):
        down[1].wait_recv()
    with SCOPE("fin1"):
        finish(1)
    with SCOPE("att0"):
        shrink_own(2)
        ours = [(0, j) for j in range(pairs)]
        ahead = [last_score(i) for i in ours[:3]]
        for i in range(2):
            last_mix(ours[i], ahead[i])
    with SCOPE("wD"):
        down[2].wait_recv()
    with SCOPE("fin2"):
        finish(2)
    with SCOPE("atts"):
        stream(ours[2:], last_score, last_mix, LOOK, ahead[2:])
        project_out(0)
    proj[0].start()
    with SCOPE("wC0"):
        proj[0].wait_recv()
    with SCOPE("ffn0"):
        n = normed_after(0)
        grow(0, n)
    with SCOPE("down0"):
        shrink_peer(0)
    down[0].start()
    with SCOPE("own0"):
        shrink_own(0)
    with SCOPE("wE"):
        down[0].wait_recv()
    with SCOPE("fin0"):
        finish(0)
    with SCOPE("backwait"):
        for r in (3, 1, 2):
            back[r].wait_recv()
    for s in range(slots):
        where = jnp.int32(0)
        for r in range(GROUP):
            where = jnp.where(own[s] == partner[r], r, where)
        live = jnp.where(entry[s] >= 0, 1.0, 0.0).astype(F32)
        block = ret[where].astype(F32)
        out_ref[s] = (block * live).astype(BF16)
    for r in range(1, GROUP):
        arrive[r].wait_send()
        back[r].wait_send()
    for r in range(GROUP):
        for c in (share, proj, down):
            c[r].wait_send()


def place(stored_ref, merged_ref, out_ref, outb_ref):
    out_ref[...] = stored_ref[...]
    outb_ref[...] = merged_ref[...]


def body(
    tokens,
    bottleneck,
    clip_lengths,
    video_blocks,
    store_map,
    norm1_gain,
    w_qkv,
    w_out,
    norm2_gain,
    w_up,
    w_down,
):
    slots, blk, width = tokens.shape
    nb = bottleneck.shape[1]
    dim = w_qkv.shape[1]
    inner = w_qkv.shape[2]
    ff = w_up.shape[1]
    pairs = inner // 128
    rows = GROUP * blk + EXTRA
    keys = (rows + 127) // 128 * 128
    vmem = pl.BlockSpec(memory_space=pltpu.VMEM)
    hbm = pl.BlockSpec(memory_space=pltpu.HBM)
    V = pltpu.VMEM
    stored, merged = pl.pallas_call(
        functools.partial(kernel, blk, nb),
        out_shape=(
            jax.ShapeDtypeStruct(tokens.shape, BF16),
            jax.ShapeDtypeStruct(bottleneck.shape, BF16),
        ),
        in_specs=[hbm] * 10,
        out_specs=(vmem, vmem),
        scratch_shapes=[
            pltpu.SMEM(video_blocks.shape, jnp.int32),
            pltpu.SMEM(store_map.shape[::-1], jnp.int32),
            V(bottleneck.shape, BF16),
            V((1, dim), F32),
            V((1, dim), F32),
            V((slots, blk, width), BF16),
            V(w_qkv.shape, BF16),
            V((2, inner, width), BF16),
            V((ff // width, dim, width), BF16),
            V((2, ff, width), BF16),
            V((GROUP - 1, blk, width), BF16),
            V((2, rows, width), BF16),
            V((EXTRA, width), F32),
            V((2, rows, inner), BF16),
            V((2 * pairs * EXTRA, inner), BF16),
            V((rows, inner), BF16),
            V((pairs, 128 + EXTRA, keys), BF16),
            V((2, pairs, 128 + EXTRA, 2 * blk), F32),
            V((2, pairs, 1, 2 * blk), F32),
            V((rows, inner), BF16),
            V((2, rows, width), BF16),
            V((2, rows, width), BF16),
            V((2, rows, width), F32),
            V((2, rows, width), BF16),
            V((rows, ff), BF16),
            V((rows, width), BF16),
            V((rows, width), BF16),
            V((rows, width), F32),
            V((GROUP - 1, blk, width), BF16),
            V((GROUP, blk, width), BF16),
            pltpu.SemaphoreType.DMA((11 + ff // width,)),
            pltpu.SemaphoreType.DMA((20,)),
            pltpu.SemaphoreType.DMA((20,)),
        ],
        compiler_params=pltpu.CompilerParams(collective_id=0, has_side_effects=True, vmem_limit_bytes=40 << 20),
        name="merge_layer",
    )(
        *(
            pltpu.with_memory_space_constraint(a, pltpu.HBM)
            for a in (
                video_blocks,
                store_map.T,
                tokens,
                bottleneck,
                norm1_gain.reshape(1, dim),
                norm2_gain.reshape(1, dim),
                w_qkv,
                w_out,
                w_up,
                w_down,
            )
        )
    )
    return pl.pallas_call(
        place,
        out_shape=(
            jax.ShapeDtypeStruct(tokens.shape, BF16),
            jax.ShapeDtypeStruct(bottleneck.shape, BF16),
        ),
        in_specs=[vmem, vmem],
        out_specs=(vmem, vmem),
        compiler_params=pltpu.CompilerParams(vmem_limit_bytes=4 << 20),
        name="place",
    )(stored, merged)


def solution(mesh):
    placed = (
        P("clip", None, "mp"),
        P("clip", None, "mp"),
        P(),
        P(),
        P(),
        P(),
        P(None, None, "mp"),
        P("mp", None),
        P(),
        P(None, "mp"),
        P("mp", None),
    )
    return jax.shard_map(
        body,
        mesh=mesh,
        in_specs=placed,
        out_specs=(P("clip", None, "mp"), P("clip", None, "mp")),
        check_vma=False,
    )
```

```python
import functools

import jax
import jax.numpy as jnp
from jax import lax
from jax.experimental import pallas as pl
from jax.experimental.pallas import tpu as pltpu
from jax.sharding import PartitionSpec as P

HEAD_DIM = 64
GROUP = 4
EPS = 1e-05
NEG = -1e30
EXTRA = 16
LOG2E = 1.4426950408889634
GELU = 0.7978845608028654
LOOK = 2
SCOPE = jax.named_scope
BF16 = jnp.bfloat16
F32 = jnp.float32


def layer_norm(halves, gain):
    x = jnp.concatenate([h.astype(F32) for h in halves], axis=1)
    mean = jnp.mean(x, axis=-1, keepdims=True)
    centred = x - mean
    moment = jnp.mean(centred * centred, axis=-1, keepdims=True)
    return (centred * lax.rsqrt(moment + EPS) * gain).astype(BF16)


def dot(a, b):
    return jnp.dot(a, b, preferred_element_type=F32)


def gelu(y):
    rate = y * (0.044715 * GELU * (y * y) + GELU)
    half = 0.5 * y
    return half + half * jnp.tanh(rate)


def kernel(
    blk,
    nb,
    video_hbm,
    map_hbm,
    tok_hbm,
    bot_hbm,
    g1_hbm,
    g2_hbm,
    wqkv_hbm,
    wout_hbm,
    wup_hbm,
    wdown_hbm,
    out_ref,
    outb_ref,
    video_ref,
    map_ref,
    bot_ref,
    g1_ref,
    g2_ref,
    tok,
    wqkv,
    wout,
    wup,
    wdown,
    snd,
    x,
    ext,
    qm,
    qb,
    k,
    vt,
    part,
    part_top,
    ctx,
    ps1,
    pr1,
    own1,
    aft,
    act,
    ps2,
    pr2,
    own2,
    fin,
    ret,
    ld_sem,
    send_sem,
    recv_sem,
):
    slots = tok.shape[0]
    width = tok.shape[2]
    pairs = vt.shape[0]
    keys = vt.shape[2]
    rows = x.shape[1]
    ff = wdown.shape[1]

    me = lax.axis_index("clip")
    core = lax.axis_index("mp")
    peer = 1 - core
    bit0 = lax.rem(me, 2)
    bit1 = lax.rem(lax.div(me, 2), 2)
    flip0 = 1 - 2 * bit0
    flip1 = 2 - 4 * bit1
    partner = [me, me + flip0, me + flip1, me + flip0 + flip1]

    barrier = pltpu.get_barrier_semaphore()
    for r in range(1, GROUP):
        pl.semaphore_signal(barrier, inc=1, device_id={"clip": partner[r]})
    pl.semaphore_signal(barrier, inc=1, device_id={"mp": peer})

    def load(i, src, dst):
        return pltpu.make_async_copy(src, dst, ld_sem.at[i])

    halves = [pl.ds(h * width, width) for h in range(2)]
    first = [
        load(0, tok_hbm, tok),
        load(1, map_hbm, map_ref),
        load(2, video_hbm, video_ref),
        load(3, bot_hbm, bot_ref),
        load(4, g1_hbm, g1_ref),
        load(5, g2_hbm, g2_ref),
    ]
    load_qkv = load(0, wqkv_hbm, wqkv)
    tiles = wup.shape[0]
    load_out = [load(1 + h, wout_hbm.at[:, halves[h]], wout.at[h]) for h in range(2)]
    load_down = [load(3 + h, wdown_hbm.at[:, halves[h]], wdown.at[h]) for h in range(2)]
    load_up = [load(5 + t, wup_hbm.at[:, pl.ds(t * width, width)], wup.at[t]) for t in range(tiles)]
    for c in first:
        c.start()

    column = lax.broadcasted_iota(jnp.int32, (1, width), 1)
    low = lax.rem(column, 2 * HEAD_DIM) < HEAD_DIM
    for j in range(pairs):
        vt[j, 2 * HEAD_DIM :] = jnp.ones((EXTRA, keys), BF16)

    for c in first:
        c.wait()
    for c in (load_qkv, *load_out, *load_up, *load_down):
        c.start()

    entry = [map_ref[s, me] for s in range(slots)]
    own = [jnp.where(e >= 0, lax.div(e, GROUP), -1) for e in entry]
    pick = []
    for r in range(GROUP):
        chosen = jnp.int32(0)
        for s in range(slots):
            chosen = jnp.where(own[s] == partner[r], s, chosen)
        pick.append(chosen)
    video = video_ref[me]
    mode = []
    for r in range(GROUP):
        m = jnp.int32(-1)
        for s in range(slots):
            e = map_ref[s, partner[r]]
            mine = (e >= 0) & (lax.div(e, GROUP) == me)
            m = jnp.where(mine, jnp.where(lax.rem(e, GROUP) < video, 0, 1), m)
        mode.append(m)

    order = [1, 2, 0]
    total = (GROUP - 1) * blk
    late = total + EXTRA
    place = [2 * blk, 0, blk, late]
    lanes = [2 * blk, 0, blk, total + 128]
    span = [pl.ds(place[0], blk + EXTRA)] + [pl.ds(place[r], blk) for r in range(1, GROUP)]

    def ici(r, src, dst, sent, got):
        return pltpu.make_async_remote_copy(
            src_ref=src,
            dst_ref=dst,
            send_sem=send_sem.at[sent + r],
            recv_sem=recv_sem.at[got + r],
            device_id={"clip": partner[r]},
        )

    def d2d(r, src, dst, sent, got):
        return pltpu.make_async_remote_copy(
            src_ref=src,
            dst_ref=dst,
            send_sem=send_sem.at[sent + r],
            recv_sem=recv_sem.at[got + r],
            device_id={"mp": peer},
        )

    half = x.at[core]
    arrive = [ici(r, snd.at[r - 1], half.at[span[r]], -1, -1) if r else None for r in range(GROUP)]
    share = [d2d(r, half.at[span[r]], half.at[span[r]], 3, 3) for r in range(GROUP)]
    proj = [d2d(r, ps1.at[:, span[r]], pr1.at[:, span[r]], 7, 7) for r in range(GROUP)]
    down = [d2d(r, ps2.at[span[r]], pr2.at[span[r]], 3, 11) for r in range(GROUP)]
    back = [ici(r, fin.at[r - 1], ret.at[r], -1, 14) if r else None for r in range(GROUP)]

    for r in range(1, GROUP):
        snd[r - 1] = tok[pick[r]]
    x[core, pl.ds(place[0], blk)] = tok[pick[0]]
    small = bot_ref[0].astype(F32)
    for i in range(EXTRA // nb):
        ext[pl.ds(i * nb, nb)] = small
    x[core, pl.ds(total, EXTRA)] = ext[...].astype(BF16)

    with SCOPE("barrier"):
        pl.semaphore_wait(barrier, GROUP)
    for r in (1, 2, 3):
        arrive[r].start()
    share[0].start()

    def seen(m, s):
        return jnp.where((mode[s] == m) & (mode[s] >= 0), 0.0, NEG).astype(F32)

    tail = lax.broadcasted_iota(jnp.int32, (EXTRA, 1), 0) < nb

    def norm(r):
        return layer_norm([x[0, span[r]], x[1, span[r]]], g1_ref[...])

    def project(r, n, then=None):
        y = dot(n, wqkv[0]) * (HEAD_DIM ** (-0.5) * LOG2E)
        y0 = jnp.where(low, y, 0.0).astype(BF16)
        y1 = jnp.where(low, 0.0, y).astype(BF16)
        qm[0, span[r]] = y0
        qm[1, span[r]] = y1
        if r == 0:
            e = y[blk:]
            head = lax.div(column, HEAD_DIM)
            for h in range(2 * pairs):
                qb[pl.ds(h * EXTRA, EXTRA)] = jnp.where(head == h, e, 0.0).astype(BF16)
        k[span[r]] = dot(n, wqkv[1]).astype(BF16)
        if then is not None:
            then()
        y = dot(n, wqkv[2])
        for j in range(pairs):
            cols = y[:, j * 128 : (j + 1) * 128]
            vt[j, :128, pl.ds(lanes[r], blk)] = cols[:blk].T.astype(BF16)
            if r == 0:
                padded = jnp.concatenate([cols[blk:], jnp.zeros((128 - EXTRA, 128), F32)], axis=0)
                vt[j, :128, pl.ds(total, 128)] = padded.T.astype(BF16)

    def column_max(s):
        m, n = s.shape
        return jnp.max(s.reshape(m // 8, 8, n), axis=0)

    def soften(s, bias, last=None, last_bias=None):
        n = s.shape[1]
        m = len(bias)
        parts = [s[p * blk : (p + 1) * blk] for p in range(m)]
        extra = jnp.where(tail, s[m * blk : m * blk + EXTRA], NEG)
        top = column_max(extra)
        for q, b in zip(parts, bias):
            top = jnp.maximum(top, column_max(q) + b)
        if last is not None:
            top = jnp.maximum(top, column_max(last) + last_bias)
        top = jnp.max(top, axis=0, keepdims=True)
        p = [jnp.exp2(q + (b - top)).astype(BF16) for q, b in zip(parts, bias)]
        p.append(jnp.exp2(extra - top).astype(BF16))
        p.append(jnp.zeros((128 - EXTRA, n), BF16))
        if last is not None:
            p.append(jnp.exp2(last + (last_bias - top)).astype(BF16))
        return jnp.concatenate(p, axis=0), top

    def merge(lasts, bias, o, top, v):
        best = top
        for q, b in zip(lasts, bias):
            best = jnp.maximum(best, jnp.max(column_max(q), axis=0, keepdims=True) + b)
        o = o * jnp.exp2(top - best)
        p = [jnp.exp2(q + (b - best)).astype(BF16) for q, b in zip(lasts, bias)]
        if len(p) > 1:
            o = o + dot(v[:, : 2 * blk], jnp.concatenate(p[:2], axis=0))
        return o + dot(v[:, split:], p[-1])

    def scores(a, b):
        return lax.dot_general(a, b, (((1,), (1,)), ((), ())), preferred_element_type=F32)

    def queries(r, j):
        at = pl.ds(place[r], blk)
        cols = slice(j * 128, (j + 1) * 128)
        return jnp.concatenate([qm[0, at, cols], qm[1, at, cols]], axis=0)

    early = pl.ds(0, late)
    split = total + 128
    own_keys = pl.ds(place[0], blk + EXTRA)
    step = lax.rem(lax.broadcasted_iota(jnp.int32, (1, 2 * pairs * EXTRA), 1), EXTRA)
    audio = (step >= nb) & (step < 2 * nb)

    def seen_small(b):
        return jnp.where(audio, seen(1, b), seen(0, b))

    def store(r, j, o):
        under = 1.0 / o[128:129]
        d = HEAD_DIM
        o = jnp.concatenate([o[:d, :blk] * under[:, :blk], o[d : 2 * d, blk:] * under[:, blk:]], axis=0)
        ctx[pl.ds(place[r], blk), j * 128 : (j + 1) * 128] = o.T.astype(BF16)

    def first_score(item):
        r, j = item
        seen_keys = own_keys if r == 0 else early
        return scores(k[seen_keys, j * 128 : (j + 1) * 128], queries(r, j))

    def first_mix(item, s):
        r, j = item
        if r == 0:
            p, top = soften(s, [seen(mode[0], 0)])
            v = vt[j, :, 2 * blk : split]
        else:
            p, top = soften(s, [seen(mode[r], b) for b in order])
            v = vt[j, :, :split]
        part_top[r, j] = top
        part[r, j] = dot(v, p)

    def last_score(item):
        r, j = item
        if r is None:
            return scores(k[early], qb[...]), scores(k[span[3]], qb[...])
        cols = slice(j * 128, (j + 1) * 128)
        q = queries(r, j)
        last = scores(k[span[3], cols], q)
        if r == 3:
            return scores(k[early, cols], q), last
        if r == 0:
            s = scores(k[: 2 * blk, cols], q)
            return s[:blk], s[blk:], last
        return (last,)

    def last_mix(item, s):
        r, j = item
        if r is None:
            p, _ = soften(s[0], [seen_small(b) for b in order], s[1], seen_small(3))
            o = [dot(vt[i], p) for i in range(pairs)]
            for i in range(pairs):
                t = (o[i][:128] * (1.0 / o[i][128:129])).T
                at = 2 * i * EXTRA
                e = jnp.where(low[:, :128], t[at : at + EXTRA], t[at + EXTRA : at + 2 * EXTRA])
                e = 0.5 * (e + pltpu.roll(e, EXTRA - nb, 0))
                ctx[pl.ds(total, EXTRA), i * 128 : (i + 1) * 128] = e.astype(BF16)
        elif r == 3:
            p, _ = soften(s[0], [seen(mode[3], b) for b in order], s[1], seen(mode[3], 3))
            store(r, j, dot(vt[j], p))
        else:
            bias = [seen(mode[r], b) for b in ((1, 2, 3) if r == 0 else (3,))]
            store(r, j, merge(s, bias, part[r, j], part_top[r, j], vt[j]))

    def stream(items, score, mix, look, ahead=()):
        waiting = dict(enumerate(ahead))
        for t in range(len(items) + look):
            if len(ahead) <= t < len(items):
                waiting[t] = score(items[t])
            if t >= look:
                mix(items[t - look], waiting.pop(t - look))

    def project_out(r):
        c = ctx[span[r]]
        for h in range(2):
            y = dot(c, wout[h])
            ps1[h, span[r]] = y.astype(BF16)
            own1[h, span[r]] = y

    def normed_after(r):
        at = span[r]
        parts = []
        for h in range(2):
            t = x[h, at].astype(F32) + (own1[h, at] + pr1[h, at].astype(F32))
            t = t.astype(BF16)
            aft[h, at] = t
            parts.append(t)
        return layer_norm(parts, g2_ref[...])

    def grow(r, n):
        for t in range(tiles):
            act[span[r], t * width : (t + 1) * width] = gelu(dot(n, wup[t])).astype(BF16)

    def shrink_peer(r):
        ps2[span[r]] = dot(act[span[r]], wdown[peer]).astype(BF16)

    def shrink_own(r):
        own2[span[r]] = dot(act[span[r]], wdown[core])

    def finish(r):
        at = span[r]
        merged = aft[core, at].astype(F32) + (own2[at] + pr2[at].astype(F32))
        if r == 0:
            ret[0] = merged[:blk].astype(BF16)
            outb_ref[0] = merged[blk : blk + nb].astype(BF16)
        else:
            fin[r - 1] = merged.astype(BF16)
            back[r].start()

    with SCOPE("w0"):
        load_qkv.wait()
        share[0].wait_recv()
    with SCOPE("project0"):
        project(0, norm(0))
        stream([(0, j) for j in range(pairs)], first_score, first_mix, LOOK)
    for r in (1, 2):
        with SCOPE("arr%d" % r):
            arrive[r].wait_recv()
        share[r].start()

    def pass_on():
        arrive[3].wait_recv()
        share[3].start()

    pl.when(core == 1)(pass_on)
    for r in (1, 2):
        with SCOPE("sh%d" % r):
            share[r].wait_recv()
    soon = [(r, j) for r in (1, 2) for j in range(pairs)]
    with SCOPE("early"):
        n1 = norm(1)
        n2 = norm(2)
        project(1, n1)
        project(2, n2)
        stream(soon, first_score, first_mix, LOOK)
    with SCOPE("arr3"):
        pl.when(core == 0)(pass_on)
    with SCOPE("ldwait"):
        for c in (*load_out, *load_up, *load_down):
            c.wait()
    with SCOPE("sh3"):
        share[3].wait_recv()
    with SCOPE("late3"):
        mine = [(3, j) for j in range(pairs)]
        ahead = []
        project(3, norm(3), lambda: ahead.extend(last_score(i) for i in mine[:LOOK]))
        stream(mine, last_score, last_mix, LOOK, ahead)
        project_out(3)
    proj[3].start()
    with SCOPE("late12"):
        stream(soon + [(None, 0)], last_score, last_mix, LOOK + 2)
        project_out(1)
    proj[1].start()
    with SCOPE("wproj3"):
        for r in range(GROUP):
            share[r].wait_send()
            if r:
                arrive[r].wait_send()
        proj[3].wait_recv()
    with SCOPE("ffn3"):
        n = normed_after(3)
        project_out(2)
        grow(3, n)
        shrink_peer(3)
    proj[2].start()
    down[3].start()
    with SCOPE("wproj1"):
        proj[1].wait_recv()
    with SCOPE("ffn1"):
        shrink_own(3)
        grow(1, normed_after(1))
        shrink_peer(1)
    down[1].start()
    with SCOPE("wB"):
        down[3].wait_recv()
    with SCOPE("fin3"):
        finish(3)
    with SCOPE("wC"):
        proj[2].wait_recv()
    with SCOPE("ffn2"):
        shrink_own(1)
        grow(2, normed_after(2))
        shrink_peer(2)
    down[2].start()
    with SCOPE("wC1"):
        down[1].wait_recv()
    with SCOPE("fin1"):
        finish(1)
    with SCOPE("att0"):
        shrink_own(2)
        ours = [(0, j) for j in range(pairs)]
        ahead = [last_score(i) for i in ours[:3]]
        for i in range(2):
            last_mix(ours[i], ahead[i])
    with SCOPE("wD"):
        down[2].wait_recv()
    with SCOPE("fin2"):
        finish(2)
    with SCOPE("atts"):
        stream(ours[2:], last_score, last_mix, LOOK, ahead[2:])
        project_out(0)
    proj[0].start()
    with SCOPE("wC0"):
        proj[0].wait_recv()
    with SCOPE("ffn0"):
        n = normed_after(0)
        grow(0, n)
        shrink_peer(0)
    down[0].start()
    with SCOPE("own0"):
        shrink_own(0)
    with SCOPE("wE"):
        down[0].wait_recv()
    with SCOPE("fin0"):
        finish(0)
    for r in range(1, GROUP):
        back[r].wait_send()
    for r in range(GROUP):
        for c in (proj, down):
            c[r].wait_send()
    with SCOPE("backwait"):
        for r in (3, 1, 2):
            back[r].wait_recv()
    with SCOPE("select"):
        for s in range(slots):
            where = jnp.int32(0)
            for r in range(GROUP):
                where = jnp.where(own[s] == partner[r], r, where)
            live = jnp.where(entry[s] >= 0, 1.0, 0.0).astype(F32)
            block = ret[where].astype(F32)
            out_ref[s] = (block * live).astype(BF16)


def place(stored_ref, merged_ref, out_hbm, outb_hbm, sem):
    copies = [
        pltpu.make_async_copy(stored_ref, out_hbm, sem.at[0]),
        pltpu.make_async_copy(merged_ref, outb_hbm, sem.at[1]),
    ]
    for c in copies:
        c.start()
    for c in copies:
        c.wait()


def body(
    tokens,
    bottleneck,
    clip_lengths,
    video_blocks,
    store_map,
    norm1_gain,
    w_qkv,
    w_out,
    norm2_gain,
    w_up,
    w_down,
):
    slots, blk, width = tokens.shape
    nb = bottleneck.shape[1]
    dim = w_qkv.shape[1]
    inner = w_qkv.shape[2]
    ff = w_up.shape[1]
    pairs = inner // 128
    rows = GROUP * blk + EXTRA
    keys = (rows + 127) // 128 * 128
    vmem = pl.BlockSpec(memory_space=pltpu.VMEM)
    hbm = pl.BlockSpec(memory_space=pltpu.HBM)
    V = pltpu.VMEM
    stored, merged = pl.pallas_call(
        functools.partial(kernel, blk, nb),
        out_shape=(
            jax.ShapeDtypeStruct(tokens.shape, BF16),
            jax.ShapeDtypeStruct(bottleneck.shape, BF16),
        ),
        in_specs=[hbm] * 10,
        out_specs=(vmem, vmem),
        scratch_shapes=[
            pltpu.SMEM(video_blocks.shape, jnp.int32),
            pltpu.SMEM(store_map.shape[::-1], jnp.int32),
            V(bottleneck.shape, BF16),
            V((1, dim), F32),
            V((1, dim), F32),
            V((slots, blk, width), BF16),
            V(w_qkv.shape, BF16),
            V((2, inner, width), BF16),
            V((ff // width, dim, width), BF16),
            V((2, ff, width), BF16),
            V((GROUP - 1, blk, width), BF16),
            V((2, rows, width), BF16),
            V((EXTRA, width), F32),
            V((2, rows, inner), BF16),
            V((2 * pairs * EXTRA, inner), BF16),
            V((rows, inner), BF16),
            V((pairs, 128 + EXTRA, keys), BF16),
            V((GROUP - 1, pairs, 128 + EXTRA, 2 * blk), F32),
            V((GROUP - 1, pairs, 1, 2 * blk), F32),
            V((rows, inner), BF16),
            V((2, rows, width), BF16),
            V((2, rows, width), BF16),
            V((2, rows, width), F32),
            V((2, rows, width), BF16),
            V((rows, ff), BF16),
            V((rows, width), BF16),
            V((rows, width), BF16),
            V((rows, width), F32),
            V((GROUP - 1, blk, width), BF16),
            V((GROUP, blk, width), BF16),
            pltpu.SemaphoreType.DMA((max(6, 5 + ff // width),)),
            pltpu.SemaphoreType.DMA((11,)),
            pltpu.SemaphoreType.DMA((18,)),
        ],
        compiler_params=pltpu.CompilerParams(collective_id=0, has_side_effects=True, vmem_limit_bytes=40 << 20),
        name="merge_layer",
    )(
        *(
            pltpu.with_memory_space_constraint(a, pltpu.HBM)
            for a in (
                video_blocks,
                store_map.T,
                tokens,
                bottleneck,
                norm1_gain.reshape(1, dim),
                norm2_gain.reshape(1, dim),
                w_qkv,
                w_out,
                w_up,
                w_down,
            )
        )
    )
    return pl.pallas_call(
        place,
        out_shape=(
            jax.ShapeDtypeStruct(tokens.shape, BF16),
            jax.ShapeDtypeStruct(bottleneck.shape, BF16),
        ),
        in_specs=[vmem, vmem],
        out_specs=(hbm, hbm),
        scratch_shapes=[pltpu.SemaphoreType.DMA((2,))],
        compiler_params=pltpu.CompilerParams(vmem_limit_bytes=4 << 20),
        name="place",
    )(stored, merged)


def solution(mesh):
    placed = (
        P("clip", None, "mp"),
        P("clip", None, "mp"),
        P(),
        P(),
        P(),
        P(),
        P(None, None, "mp"),
        P("mp", None),
        P(),
        P(None, "mp"),
        P("mp", None),
    )
    return jax.shard_map(
        body,
        mesh=mesh,
        in_specs=placed,
        out_specs=(P("clip", None, "mp"), P("clip", None, "mp")),
        check_vma=False,
    )
```
